32 devices in a mesh: seq: 8 (over z, core), head: 4 (over y, x).
Axes of the slice: x: 2, y: 2, z: 4, core: 2. Of those that a mesh axis runs over, the one named last changes fastest.
Arguments:
- tokens: bfloat16 [1024, 4096], P('seq', 'head'), may hold values from -6 to 6
- w_query: bfloat16 [4096, 4096], P(None, 'head'), may hold values from -0.09375 to 0.09375
- w_key: bfloat16 [4096, 4096], P(None, 'head'), may hold values from -0.09375 to 0.09375
- w_value: bfloat16 [4096, 4096], P(None, 'head'), may hold values from -0.09375 to 0.09375
- upstream: bfloat16 [1024, 4096], P('seq', 'head'), may hold values from -6 to 6
- log_decay: float32 [1024, 32], P('seq', 'head'), may hold values from -1 to 0, as said below
- segment: int32 [1024], replicated, may hold values from 0 to 7, never falling along the last dimension, each value on 1 to 256 neighbouring positions
Outputs:
- grad_query: bfloat16 [4096, 4096], P('seq', 'head')
- grad_key: bfloat16 [4096, 4096], P('seq', 'head')
- grad_value: bfloat16 [4096, 4096], P('seq', 'head')
The draws below stay inside these ranges and needn't reach their ends.
Inputs may be any that keep to these rules, and one draw needn't show every extreme that they name: log_decay is negative. `segment`: document ids never fall along the tokens; each document holds 1 to 256 tokens.
All inputs are finite; a program needn't handle non-finite values.
Results may differ from the reference program's by a relative error of at most 0.02.
Values may be sent and summed in bfloat16 or wider, within the bound.
No kernel may reach another device: no remote copies, remote signals or barrier semaphores. Data moves between devices by JAX's collectives and lax.ppermute only.
A program may use at most 64 MiB of HBM per device.

```python
import math
import jax
import jax.numpy as jnp
import numpy as np
from jax import lax

D = 4096
HEAD_COUNT = 32
HEAD = 128
TOK_DEV = 128
DOCS = 8
TOKEN_COUNT = 1024
N_SEQ = 8


def draw_log_decay(key, part):
    document_lanes = jax.random.split(key, 6)
    fast_share = 0.5
    fast = jax.random.uniform(document_lanes[0], (HEAD_COUNT,)) < fast_share
    slow_rate = jax.random.uniform(document_lanes[1], (HEAD_COUNT,), minval=0.1, maxval=0.4) * math.log(10.0) / TOKEN_COUNT
    fast_rate = 1.0 / jax.random.uniform(document_lanes[2], (HEAD_COUNT,), minval=30.0, maxval=50.0)
    decay_rate = jnp.where(fast, fast_rate, slow_rate)
    coarse_estimate = jnp.exp(jax.random.uniform(document_lanes[3], (TOKEN_COUNT, HEAD_COUNT), minval=-math.log(2.0), maxval=math.log(2.0)))
    decay_jump = jax.random.uniform(document_lanes[4], (TOKEN_COUNT, HEAD_COUNT)) < 2.0 / TOKEN_COUNT
    feature_depth = jax.random.uniform(document_lanes[5], (TOKEN_COUNT, HEAD_COUNT), minval=0.22, maxval=0.69)
    return (-(decay_rate[None, :] * coarse_estimate) - jnp.where(decay_jump, feature_depth, 0.0)).astype(jnp.float32)


def strengthened(values, stream_key, source, target, parts, factor):
    owner, partner = [(jnp.arange(values.shape[dim]) // (values.shape[dim] // parts)).reshape([-1 if axis == dim else 1 for axis in range(values.ndim)]) for dim in (source, target)]
    chosen = jax.random.permutation(stream_key, parts)[partner]
    strong = (owner == chosen) | (owner == (partner + parts // 2) % parts)
    return jnp.where(strong, factor * values, values)


def steps_of(key, extent, cuts, smallest, high):
    def one(axis_at, blocks):
        draws = jax.random.uniform(jax.random.fold_in(jax.random.fold_in(key, 6), axis_at), (blocks,), jnp.float32, smallest / len(cuts), high / len(cuts))
        return jnp.repeat(jnp.exp(draws), extent[axis_at] // blocks).reshape((-1,) + (1,) * (len(extent) - axis_at - 1))

    gain = one(*cuts[0])
    for cut in cuts[1:]:
        gain = gain * one(*cut)
    return gain


def profile(count, total, limit, lean):
    weights = [(1 << 20) // math.isqrt(rank ** lean) + 1 for rank in range(2, count + 1)]
    surplus, holding = total - limit - (count - 1), [1] * (count - 1)
    while surplus > 0:
        movable = [i for i in range(count - 1) if holding[i] < limit]
        pool, remaining = sum([weights[i] for i in movable]), surplus
        for i in movable:
            more = min(limit - holding[i], max(1, remaining * weights[i] // pool), surplus)
            holding[i] = holding[i] + more
            surplus = surplus - more
    return np.array([limit] + holding)


def uneven(rng, number_of, total, reach, lean):
    if number_of == 2:
        one = jax.random.randint(rng, (), max(1, total - reach), min(reach, total - 1) + 1)
        return jnp.stack([one, total - one])
    tallies = jnp.asarray(profile(number_of, total, reach, lean), jnp.int32)
    pairs = (number_of - 1) // 2
    donor, taker = tallies[1:1 + 2 * pairs:2], tallies[2:2 + 2 * pairs:2]
    room = jnp.minimum(donor - 1, reach - taker)
    moved = jax.random.randint(jax.random.fold_in(rng, 1), (pairs,), 0, 1 << 20) % (room + 1)
    tallies = tallies.at[1:1 + 2 * pairs:2].set(donor - moved).at[2:2 + 2 * pairs:2].set(taker + moved)
    return tallies[jax.random.permutation(jax.random.fold_in(rng, 2), number_of)]


def scatter_about(own_key, dims, scale, reach, cuts=(), kind=jnp.bfloat16):
    result = scale * jax.random.normal(own_key, dims, jnp.float32)
    if cuts:
        result = result * steps_of(own_key, dims, cuts, -0.22, 0.18)
    return jnp.clip(result, -reach, reach).astype(kind)


def heavy_noise(rng, extent, scale, reach, shards, heavy, held_as=jnp.bfloat16):
    values = scale * jax.random.normal(rng, extent, jnp.float32)
    if shards:
        values = values * steps_of(rng, extent, shards, -0.22, 0.18)
    return jnp.clip(strengthened(values, jax.random.fold_in(rng, 3), *heavy), -reach, reach).astype(held_as)


def setup_inputs(seed: int = 0) -> dict:
    key_list = jax.random.split(jax.random.key(seed), 8)
    return {
        "tokens": heavy_noise(key_list[0], (TOKEN_COUNT, D), 1.0, 6.0, ((0, 8), (1, 4)), (0, 1, 8, 2.0)),
        "w_query": scatter_about(key_list[1], (D, HEAD_COUNT * HEAD), D ** -0.5, 0.09375, ((1, 4),)),
        "w_key": scatter_about(key_list[2], (D, HEAD_COUNT * HEAD), D ** -0.5, 0.09375, ((1, 4),)),
        "w_value": scatter_about(key_list[3], (D, HEAD_COUNT * HEAD), D ** -0.5, 0.09375, ((1, 4),)),
        "upstream": scatter_about(key_list[4], (TOKEN_COUNT, HEAD_COUNT * HEAD), 1.0, 6.0, ((0, 8), (1, 4))),
        "log_decay": draw_log_decay(jax.random.fold_in(key_list[7], 71), 0),
        "segment": jnp.searchsorted(jnp.cumsum(uneven(key_list[6], DOCS, TOKEN_COUNT, TOKEN_COUNT // 4, 0)), jnp.arange(TOKEN_COUNT), side="right").astype(jnp.int32),
    }


def rounded(array):
    return lax.optimization_barrier(array.astype(jnp.bfloat16)).astype(jnp.float32)

def block_factors(log_rates, segs, previous):
    log_sum = jnp.cumsum(log_rates, axis=0)
    last_sum = log_sum[-1]
    last_seg = segs[-1]
    state_entering = jnp.where((segs == previous)[:, None], jnp.exp(log_sum), 0.0)
    state_leaving = jnp.where((segs == last_seg)[:, None], jnp.exp(last_sum[None, :] - log_sum), 0.0)
    carry_decay = jnp.where(last_seg == previous, jnp.exp(last_sum), 0.0)
    places = jnp.arange(segs.shape[0], dtype=jnp.int32)
    same = (segs[:, None] == segs[None, :]) & (places[:, None] >= places[None, :])
    spread = log_sum.T[:, :, None] - log_sum.T[:, None, :]
    decay_mat = jnp.where(same[None], HEAD ** (-0.5) * jnp.exp(jnp.where(same[None], spread, 0.0)), 0.0)
    return (state_entering, state_leaving, carry_decay, decay_mat)

def summaries(block):
    query, key_rows, value_rows, upstream, log_rates, segs, previous = block
    state_entering, state_leaving, carry_decay, decay_mat = block_factors(log_rates, segs, previous)
    scale = HEAD ** (-0.5)
    weighted_keys = rounded(scale * state_leaving[:, :, None] * key_rows.astype(jnp.float32))
    segment_state = jnp.einsum('bdw,bdq->dwq', weighted_keys, value_rows.astype(jnp.float32), precision=lax.Precision.HIGHEST)
    weighted_queries = rounded(scale * state_entering[:, :, None] * query.astype(jnp.float32))
    following_state = jnp.einsum('bdw,bdq->dwq', weighted_queries, upstream.astype(jnp.float32), precision=lax.Precision.HIGHEST)
    return (carry_decay, segment_state, following_state)

def block_grads(block):
    query, key_rows, value_rows, upstream, log_rates, segs, previous, arriving_state, backward_state = block
    state_entering, state_leaving, carry_decay, decay_mat = block_factors(log_rates, segs, previous)
    query_rows_float = query.astype(jnp.float32)
    key_rows_float = key_rows.astype(jnp.float32)
    value_rows_float = value_rows.astype(jnp.float32)
    upstream_float = upstream.astype(jnp.float32)
    upper_limit = lax.Precision.HIGHEST
    attention_query_key = rounded(decay_mat * jnp.einsum('thd,shd->hts', query_rows_float, key_rows_float, precision=upper_limit))
    attention_upstream = rounded(decay_mat * jnp.einsum('thd,shd->hts', upstream_float, value_rows_float, precision=upper_limit))
    query_gradient = jnp.einsum('wcz,zwm->cwm', attention_upstream, key_rows_float, precision=upper_limit) + state_entering[:, :, None] * jnp.einsum('pzo,zao->pza', upstream_float, arriving_state, precision=upper_limit)
    key_gradient = jnp.einsum('voi,ovw->ivw', attention_upstream, query_rows_float, precision=upper_limit) + state_leaving[:, :, None] * jnp.einsum('ixz,xqz->ixq', value_rows_float, backward_state, precision=upper_limit)
    value_gradient = jnp.einsum('voi,ovw->ivw', attention_query_key, upstream_float, precision=upper_limit) + state_leaving[:, :, None] * jnp.einsum('dqg,qgf->dqf', key_rows_float, backward_state, precision=upper_limit)
    return (query_gradient.astype(jnp.bfloat16), key_gradient.astype(jnp.bfloat16), value_gradient.astype(jnp.bfloat16))

def reference(tokens, w_query, w_key, w_value, upstream, log_decay, segment):
    blocks = N_SEQ
    width = HEAD_COUNT * HEAD

    def project(weight):
        product = jnp.dot(tokens, weight, preferred_element_type=jnp.float32).astype(jnp.bfloat16)
        return product.reshape(blocks, TOK_DEV, HEAD_COUNT, HEAD)
    query = project(w_query)
    key_rows = project(w_key)
    value_rows = project(w_value)
    grads_up = upstream.reshape(blocks, TOK_DEV, HEAD_COUNT, HEAD)
    rates = log_decay.reshape(blocks, TOK_DEV, HEAD_COUNT)
    segs = segment.reshape(blocks, TOK_DEV)
    previous = jnp.concatenate([jnp.full((1,), -1, jnp.int32), segs[:-1, -1]])
    decays, local_states, later_states = lax.map(summaries, (query, key_rows, value_rows, grads_up, rates, segs, previous))

    def forward(state, item):
        decay, segment_state = item
        return (decay[:, None, None] * state + segment_state, state)
    zeros = jnp.zeros((HEAD_COUNT, HEAD, HEAD), jnp.float32)
    _, arriving_state = lax.scan(forward, zeros, (decays, local_states))
    _, backward_state = lax.scan(forward, zeros, (decays, later_states), reverse=True)
    query_gradient, key_gradient, value_gradient = lax.map(block_grads, (query, key_rows, value_rows, grads_up, rates, segs, previous, arriving_state, backward_state))

    def weight_grad(grads):
        flat = grads.reshape(TOKEN_COUNT, width)
        return jnp.dot(tokens.T, flat, preferred_element_type=jnp.float32).astype(jnp.bfloat16)
    return (weight_grad(query_gradient), weight_grad(key_gradient), weight_grad(value_gradient))
```

```python
import jax
import jax.numpy as jnp
from jax import lax
from jax.experimental import pallas as pl
from jax.experimental.pallas import tpu as pltpu
from jax.sharding import PartitionSpec as P

HEAD = 128
SCALE = HEAD ** (-0.5)
CONTRACT_FIRST = (((0,), (0,)), ((), ()))
CONTRACT_LAST = (((1,), (1,)), ((), ()))
VMEM = pl.BlockSpec(memory_space=pltpu.VMEM)


def dot(a, b, dims=(((1,), (0,)), ((), ()))):
    return lax.dot_general(a, b, dims, preferred_element_type=jnp.float32)


def factors(sums_ref, meta_ref, head):
    rows = meta_ref.shape[1]
    along = jnp.broadcast_to(sums_ref[head : head + 1, :], (rows, rows))
    down = along.T
    seg_along = jnp.broadcast_to(meta_ref[0:1, :], (rows, rows))
    seg_down = seg_along.T
    return along, down, seg_along, seg_down


def inflow_tile(down, seg_down, meta_ref):
    return jnp.where(seg_down == meta_ref[1:2, :], jnp.exp(down), 0.0)


def outflow_tile(down, seg_down, sums_ref, meta_ref, head):
    last = sums_ref[head : head + 1, -1:]
    return jnp.where(seg_down == meta_ref[0:1, -1:], jnp.exp(last - down), 0.0)


def states_kernel(query, keys, values, upstream, sums, meta, local_state, later_state):
    for h in range(sums.shape[0]):
        at = slice(h * HEAD, (h + 1) * HEAD)
        _, down, _, seg_down = factors(sums, meta, h)
        out = outflow_tile(down, seg_down, sums, meta, h)
        b = (SCALE * out * keys[:, at].astype(jnp.float32)).astype(jnp.bfloat16)
        local_state[h] = dot(b, values[:, at], CONTRACT_FIRST).astype(jnp.bfloat16)
        into = inflow_tile(down, seg_down, meta)
        c = (SCALE * into * query[:, at].astype(jnp.float32)).astype(jnp.bfloat16)
        later_state[h] = dot(c, upstream[:, at], CONTRACT_FIRST).astype(jnp.bfloat16)


def intra_kernel(query, keys, values, upstream, sums, meta, part_q, part_k, part_v):
    rows = meta.shape[1]
    causal = lax.broadcasted_iota(jnp.int32, (rows, rows), 0) >= lax.broadcasted_iota(
        jnp.int32, (rows, rows), 1
    )
    for h in range(sums.shape[0]):
        at = slice(h * HEAD, (h + 1) * HEAD)
        along, down, seg_along, seg_down = factors(sums, meta, h)
        same = causal & (seg_along == seg_down)
        decay = jnp.where(same, SCALE * jnp.exp(jnp.where(same, down - along, 0.0)), 0.0)
        q, k, v, u = query[:, at], keys[:, at], values[:, at], upstream[:, at]
        attn_qk = (decay * dot(q, k, CONTRACT_LAST)).astype(jnp.bfloat16)
        attn_up = (decay * dot(u, v, CONTRACT_LAST)).astype(jnp.bfloat16)
        part_q[:, at] = dot(attn_up, k)
        part_k[:, at] = dot(attn_up, q, CONTRACT_FIRST)
        part_v[:, at] = dot(attn_qk, u, CONTRACT_FIRST)


def chained(states, carries, head):
    total = states[-1][head].astype(jnp.float32)
    for state, carry in zip(states[-2::-1], carries[::-1]):
        total = state[head].astype(jnp.float32) + carry[head : head + 1, :] * total
    return total.astype(jnp.bfloat16)


def make_inter_kernel(reach):
    def inter_kernel(*refs):
        keys, values, upstream, sums, meta, part_q, part_k, part_v = refs[:8]
        rest = refs[8:-3]
        earlier, later = rest[:reach], rest[reach : 2 * reach]
        carry_back = rest[2 * reach : 3 * reach - 1]
        carry_ahead = rest[3 * reach - 1 :]
        grad_q, grad_k, grad_v = refs[-3:]
        for h in range(sums.shape[0]):
            at = slice(h * HEAD, (h + 1) * HEAD)
            _, down, _, seg_down = factors(sums, meta, h)
            out = outflow_tile(down, seg_down, sums, meta, h)
            into = inflow_tile(down, seg_down, meta)
            incoming = chained(earlier, carry_back, h)
            returning = chained(later, carry_ahead, h)
            u, v, k = upstream[:, at], values[:, at], keys[:, at]
            grad_v[:, at] = (part_v[:, at] + out * dot(k, returning)).astype(jnp.bfloat16)
            grad_k[:, at] = (
                part_k[:, at] + out * dot(v, returning, CONTRACT_LAST)
            ).astype(jnp.bfloat16)
            grad_q[:, at] = (
                part_q[:, at] + into * dot(u, incoming, CONTRACT_LAST)
            ).astype(jnp.bfloat16)

    return inter_kernel


def call(kernel, outs, operands, flops):
    return pl.pallas_call(
        kernel,
        out_shape=outs,
        in_specs=[VMEM] * len(operands),
        out_specs=[VMEM] * len(outs),
        cost_estimate=pl.CostEstimate(flops=flops, bytes_accessed=4 << 20, transcendentals=0),
    )(*operands)


def shifted(x, offset, count):
    pairs = [(i, i + offset) for i in range(count) if 0 <= i + offset < count]
    return lax.ppermute(x, "seq", pairs)


def local(tokens, w_query, w_key, w_value, upstream, log_decay, segment):
    rows, part_width = tokens.shape
    width = w_query.shape[1]
    heads = width // HEAD
    head_count, count = lax.axis_size("head"), lax.axis_size("seq")
    my_head, my_index = lax.axis_index("head"), lax.axis_index("seq")

    token_parts = [tokens] + [
        lax.ppermute(tokens, "head", [(i, i ^ k) for i in range(head_count)])
        for k in range(1, head_count)
    ]

    first = my_index * rows
    segs = lax.dynamic_slice_in_dim(segment, first, rows)
    before = lax.dynamic_slice_in_dim(segment, jnp.maximum(first - 1, 0), 1)[0]
    previous = jnp.where(my_index > 0, before, jnp.int32(-1))
    upper = jnp.triu(jnp.ones((rows, rows), jnp.float32))
    sums = lax.dot_general(
        log_decay, upper, CONTRACT_FIRST, precision=lax.Precision.HIGHEST,
        preferred_element_type=jnp.float32,
    )
    carry = jnp.where(segs[-1] == previous, jnp.exp(sums[:, -1:]), 0.0)
    carry = jnp.broadcast_to(carry, (heads, HEAD))
    meta = jnp.stack([segs, jnp.full_like(segs, previous)]).astype(jnp.float32)

    longest = segment.shape[0] // 4
    reach = min((longest - 1) // rows + 1, count - 1)
    carry_back = [shifted(carry, j, count) for j in range(1, reach)]
    carry_ahead = [shifted(carry, -j, count) for j in range(1, reach)]

    def project(weight):
        total = None
        for k, part in enumerate(token_parts):
            start = (my_head ^ k) * part_width
            term = dot(part, lax.dynamic_slice_in_dim(weight, start, part_width))
            total = term if total is None else total + term
        return total.astype(jnp.bfloat16)

    query, keys, values = project(w_query), project(w_key), project(w_value)

    square = jax.ShapeDtypeStruct((heads, HEAD, HEAD), jnp.bfloat16)
    flat_float = jax.ShapeDtypeStruct((rows, width), jnp.float32)
    flat = jax.ShapeDtypeStruct((rows, width), jnp.bfloat16)
    one = 2 * rows * HEAD * width
    shared = [query, keys, values, upstream, sums, meta]
    local_state, later_state = call(states_kernel, [square] * 2, shared, 2 * one)
    earlier = [shifted(local_state, j, count) for j in range(1, reach + 1)]
    later = [shifted(later_state, -j, count) for j in range(1, reach + 1)]
    parts = call(intra_kernel, [flat_float] * 3, shared, 5 * one)

    chips = count // 2
    chip, core = my_index // 2, my_index % 2
    own_width = part_width * head_count // count
    per_part = part_width // own_width
    stacked = jnp.stack(token_parts)

    def columns_for(place):
        return lax.dynamic_slice(
            stacked,
            ((place // per_part) ^ my_head, 0, (place % per_part) * own_width),
            (1, rows, own_width),
        )[0]

    columns = []
    for d in range(chips):
        for p in range(2):
            block = columns_for(2 * ((chip + d) % chips) + (core ^ p))
            if d or p:
                block = lax.ppermute(
                    block, "seq",
                    [(i, 2 * ((i // 2 + d) % chips) + ((i % 2) ^ p)) for i in range(count)],
                )
            columns.append(block)
    columns = jnp.concatenate(columns, axis=0)

    grads = call(
        make_inter_kernel(reach), [flat] * 3,
        [keys, values, upstream, sums, meta, *parts, *earlier, *later, *carry_back, *carry_ahead],
        3 * one,
    )

    ahead = [(i, (i + 2) % count) for i in range(count)]
    behind = [(i, (i - 2) % count) for i in range(count)]
    partner = [(i, i ^ 1) for i in range(count)]

    def everything(grad):
        found = {0: grad}
        right = left = grad
        middle = chips // 2
        for d in range(1, middle):
            right = lax.ppermute(right, "seq", ahead)
            left = lax.ppermute(left, "seq", behind)
            found[d], found[chips - d] = right, left
        half = rows // 2
        upper_half = lax.ppermute(right[:half], "seq", ahead)
        lower_half = lax.ppermute(left[half:], "seq", behind)
        found[middle] = jnp.concatenate([upper_half, lower_half], axis=0)
        blocks = []
        for d in range(chips):
            blocks += [found[d], lax.ppermute(found[d], "seq", partner)]
        return jnp.concatenate(blocks, axis=0)

    return tuple(
        dot(columns, everything(grad), CONTRACT_FIRST).astype(jnp.bfloat16) for grad in grads
    )


def solution(mesh):
    placed = (
        P("seq", "head"),
        P(None, "head"),
        P(None, "head"),
        P(None, "head"),
        P("seq", "head"),
        P("seq", "head"),
        P(),
    )
    return jax.shard_map(
        local,
        mesh=mesh,
        in_specs=placed,
        out_specs=(P("seq", "head"), P("seq", "head"), P("seq", "head")),
        check_vma=False,
    )
```

```python
import jax
import jax.numpy as jnp
from jax import lax
from jax.experimental import pallas as pl
from jax.experimental.pallas import tpu as pltpu
from jax.sharding import PartitionSpec as P

HEAD = 128
SCALE = HEAD ** (-0.5)
EXTRA = 16
CONTRACT_FIRST = (((0,), (0,)), ((), ()))
CONTRACT_LAST = (((1,), (1,)), ((), ()))
VMEM = pl.BlockSpec(memory_space=pltpu.VMEM)


def dot(a, b, dims=(((1,), (0,)), ((), ()))):
    return lax.dot_general(a, b, dims, preferred_element_type=jnp.float32)


def factors(sums_ref, meta_ref, head):
    rows = meta_ref.shape[1]
    along = jnp.broadcast_to(sums_ref[head : head + 1, :], (rows, rows))
    down = along.T
    seg_along = jnp.broadcast_to(meta_ref[0:1, :], (rows, rows))
    seg_down = seg_along.T
    return along, down, seg_along, seg_down


def inflow_tile(down, seg_down, meta_ref):
    return jnp.where(seg_down == meta_ref[1:2, :], jnp.exp(down), 0.0)


def outflow_tile(down, seg_down, sums_ref, meta_ref, head):
    last = sums_ref[head : head + 1, -1:]
    return jnp.where(seg_down == meta_ref[0:1, -1:], jnp.exp(last - down), 0.0)


def states_kernel(query, keys, values, upstream, sums, meta, local_state, later_state):
    for h in range(sums.shape[0]):
        at = slice(h * HEAD, (h + 1) * HEAD)
        _, down, _, seg_down = factors(sums, meta, h)
        out = outflow_tile(down, seg_down, sums, meta, h)
        b = (SCALE * out * keys[:, at].astype(jnp.float32)).astype(jnp.bfloat16)
        local_state[h, :HEAD] = dot(b, values[:, at], CONTRACT_FIRST).astype(jnp.bfloat16)
        into = inflow_tile(down, seg_down, meta)
        c = (SCALE * into * query[:, at].astype(jnp.float32)).astype(jnp.bfloat16)
        later_state[h, :HEAD] = dot(c, upstream[:, at], CONTRACT_FIRST).astype(jnp.bfloat16)
        carry = jnp.where(
            meta[0:1, -1:] == meta[1:2, -1:], jnp.exp(sums[h : h + 1, -1:]), 0.0
        )
        carry = jnp.broadcast_to(carry, (EXTRA, HEAD)).astype(jnp.bfloat16)
        local_state[h, HEAD:] = carry
        later_state[h, HEAD:] = carry


def intra_kernel(query, keys, values, upstream, sums, meta, part_q, part_k, part_v):
    rows = meta.shape[1]
    causal = lax.broadcasted_iota(jnp.int32, (rows, rows), 0) >= lax.broadcasted_iota(
        jnp.int32, (rows, rows), 1
    )
    for h in range(sums.shape[0]):
        at = slice(h * HEAD, (h + 1) * HEAD)
        along, down, seg_along, seg_down = factors(sums, meta, h)
        same = causal & (seg_along == seg_down)
        decay = jnp.where(same, SCALE * jnp.exp(jnp.where(same, down - along, 0.0)), 0.0)
        q, k, v, u = query[:, at], keys[:, at], values[:, at], upstream[:, at]
        attn_qk = (decay * dot(q, k, CONTRACT_LAST)).astype(jnp.bfloat16)
        attn_up = (decay * dot(u, v, CONTRACT_LAST)).astype(jnp.bfloat16)
        part_q[:, at] = dot(attn_up, k)
        part_k[:, at] = dot(attn_up, q, CONTRACT_FIRST)
        part_v[:, at] = dot(attn_qk, u, CONTRACT_FIRST)


def chained(states, head):
    total = states[-1][head, :HEAD].astype(jnp.float32)
    for state in states[-2::-1]:
        own = state[head].astype(jnp.float32)
        total = own[:HEAD] + own[HEAD : HEAD + 1] * total
    return total.astype(jnp.bfloat16)


def make_inter_kernel(reach):
    def inter_kernel(*refs):
        keys, values, upstream, sums, meta, part_q, part_k, part_v = refs[:8]
        rest = refs[8:-1]
        earlier, later = rest[:reach], rest[reach:]
        grads = refs[-1]
        for h in range(sums.shape[0]):
            at = slice(h * HEAD, (h + 1) * HEAD)
            _, down, _, seg_down = factors(sums, meta, h)
            out = outflow_tile(down, seg_down, sums, meta, h)
            into = inflow_tile(down, seg_down, meta)
            incoming = chained(earlier, h)
            returning = chained(later, h)
            u, v, k = upstream[:, at], values[:, at], keys[:, at]
            grads[2, :, at] = (part_v[:, at] + out * dot(k, returning)).astype(jnp.bfloat16)
            grads[1, :, at] = (
                part_k[:, at] + out * dot(v, returning, CONTRACT_LAST)
            ).astype(jnp.bfloat16)
            grads[0, :, at] = (
                part_q[:, at] + into * dot(u, incoming, CONTRACT_LAST)
            ).astype(jnp.bfloat16)

    return inter_kernel


def call(kernel, outs, operands, flops):
    return pl.pallas_call(
        kernel,
        out_shape=outs,
        in_specs=[VMEM] * len(operands),
        out_specs=[VMEM] * len(outs),
        cost_estimate=pl.CostEstimate(flops=flops, bytes_accessed=4 << 20, transcendentals=0),
    )(*operands)


def shifted(x, offset, count):
    pairs = [(i, i + offset) for i in range(count) if 0 <= i + offset < count]
    return lax.ppermute(x, "seq", pairs)


def local(tokens, w_query, w_key, w_value, upstream, log_decay, segment):
    rows, part_width = tokens.shape
    width = w_query.shape[1]
    heads = width // HEAD
    head_count, count = lax.axis_size("head"), lax.axis_size("seq")
    my_head, my_index = lax.axis_index("head"), lax.axis_index("seq")

    token_parts = [tokens] + [
        lax.ppermute(tokens, "head", [(i, i ^ k) for i in range(head_count)])
        for k in range(1, head_count)
    ]

    first = my_index * rows
    segs = lax.dynamic_slice_in_dim(segment, first, rows)
    before = lax.dynamic_slice_in_dim(segment, jnp.maximum(first - 1, 0), 1)[0]
    previous = jnp.where(my_index > 0, before, jnp.int32(-1))
    upper = jnp.triu(jnp.ones((rows, rows), jnp.float32))
    sums = lax.dot_general(
        log_decay, upper, CONTRACT_FIRST, precision=lax.Precision.HIGHEST,
        preferred_element_type=jnp.float32,
    )
    meta = jnp.stack([segs, jnp.full_like(segs, previous)]).astype(jnp.float32)

    longest = segment.shape[0] // 4
    reach = min((longest - 1) // rows + 1, count - 1)

    def project(weight):
        total = None
        for k, part in enumerate(token_parts):
            start = (my_head ^ k) * part_width
            term = dot(part, lax.dynamic_slice_in_dim(weight, start, part_width))
            total = term if total is None else total + term
        return total.astype(jnp.bfloat16)

    query, keys, values = project(w_query), project(w_key), project(w_value)

    square = jax.ShapeDtypeStruct((heads, HEAD + EXTRA, HEAD), jnp.bfloat16)
    flat_float = jax.ShapeDtypeStruct((rows, width), jnp.float32)
    triple = jax.ShapeDtypeStruct((3, rows, width), jnp.bfloat16)
    one = 2 * rows * HEAD * width
    shared = [query, keys, values, upstream, sums, meta]
    local_state, later_state = call(states_kernel, [square] * 2, shared, 2 * one)
    earlier = [shifted(local_state, j, count) for j in range(1, reach + 1)]
    later = [shifted(later_state, -j, count) for j in range(1, reach + 1)]
    parts = call(intra_kernel, [flat_float] * 3, shared, 5 * one)

    chips = count // 2
    chip, core = my_index // 2, my_index % 2
    own_width = part_width * head_count // count
    per_part = part_width // own_width
    stacked = jnp.stack(token_parts)

    def columns_for(place):
        return lax.dynamic_slice(
            stacked,
            ((place // per_part) ^ my_head, 0, (place % per_part) * own_width),
            (1, rows, own_width),
        )[0]

    partner = [(i, i ^ 1) for i in range(count)]
    places = [2 * ((chip + d) % chips) for d in range(chips)]
    kept = [columns_for(place + core) for place in places]
    given = jnp.stack([columns_for(place + 1 - core) for place in places])
    taken = lax.ppermute(given, "seq", partner)
    columns = []
    for d in range(chips):
        block = jnp.concatenate([kept[d], taken[d]], axis=0)
        if d:
            block = lax.ppermute(block, "seq", [(i, (i + 2 * d) % count) for i in range(count)])
        columns.append(block)

    (grads,) = call(
        make_inter_kernel(reach), [triple],
        [keys, values, upstream, sums, meta, *parts, *earlier, *later],
        3 * one,
    )
    columns, grads = lax.optimization_barrier((columns, grads))

    ahead = [(i, (i + 2) % count) for i in range(count)]
    behind = [(i, (i - 2) % count) for i in range(count)]
    middle = chips // 2
    found = {0: grads}
    right = left = grads
    for d in range(1, middle):
        right = lax.ppermute(right, "seq", ahead)
        left = lax.ppermute(left, "seq", behind)
        found[d], found[chips - d] = right, left
    half = rows // 2
    halves = [
        lax.ppermute(right[:, :half], "seq", ahead),
        lax.ppermute(left[:, half:], "seq", behind),
    ]
    found = {d: [x, lax.ppermute(x, "seq", partner)] for d, x in found.items()}
    halves = [(x, lax.ppermute(x, "seq", partner)) for x in halves]
    near = sorted(found)
    near_columns = jnp.concatenate([columns[d] for d in near], axis=0)

    outs = []
    for i in range(3):
        block = jnp.concatenate([x[i] for d in near for x in found[d]], axis=0)
        total = dot(near_columns, block, CONTRACT_FIRST)
        far = jnp.concatenate([x[p][i] for p in range(2) for x in halves], axis=0)
        total = total + dot(columns[middle], far, CONTRACT_FIRST)
        outs.append(total.astype(jnp.bfloat16))
    return tuple(outs)


def solution(mesh):
    placed = (
        P("seq", "head"),
        P(None, "head"),
        P(None, "head"),
        P(None, "head"),
        P("seq", "head"),
        P("seq", "head"),
        P(),
    )
    return jax.shard_map(
        local,
        mesh=mesh,
        in_specs=placed,
        out_specs=(P("seq", "head"), P("seq", "head"), P("seq", "head")),
        check_vma=False,
    )
```

```python
import jax
import jax.numpy as jnp
from jax import lax
from jax.experimental import pallas as pl
from jax.experimental.pallas import tpu as pltpu
from jax.sharding import PartitionSpec as P

HEAD = 128
SCALE = HEAD ** (-0.5)
EXTRA = 16
CONTRACT_FIRST = (((0,), (0,)), ((), ()))
CONTRACT_LAST = (((1,), (1,)), ((), ()))
VMEM = pl.BlockSpec(memory_space=pltpu.VMEM)


def dot(a, b, dims=(((1,), (0,)), ((), ()))):
    return lax.dot_general(a, b, dims, preferred_element_type=jnp.float32)


def factors(sums_ref, meta_ref, head):
    rows = meta_ref.shape[1]
    along = jnp.broadcast_to(sums_ref[head : head + 1, :], (rows, rows))
    down = along.T
    seg_along = jnp.broadcast_to(meta_ref[0:1, :], (rows, rows))
    seg_down = seg_along.T
    return along, down, seg_along, seg_down


def inflow_tile(down, seg_down, meta_ref):
    return jnp.where(seg_down == meta_ref[1:2, :], jnp.exp(down), 0.0)


def outflow_tile(down, seg_down, sums_ref, meta_ref, head):
    last = sums_ref[head : head + 1, -1:]
    return jnp.where(seg_down == meta_ref[0:1, -1:], jnp.exp(last - down), 0.0)


def states_kernel(query, keys, values, upstream, sums, meta, local_state, later_state):
    for h in range(sums.shape[0]):
        at = slice(h * HEAD, (h + 1) * HEAD)
        _, down, _, seg_down = factors(sums, meta, h)
        out = outflow_tile(down, seg_down, sums, meta, h)
        b = (SCALE * out * keys[:, at].astype(jnp.float32)).astype(jnp.bfloat16)
        local_state[h, :HEAD] = dot(b, values[:, at], CONTRACT_FIRST).astype(jnp.bfloat16)
        into = inflow_tile(down, seg_down, meta)
        c = (SCALE * into * query[:, at].astype(jnp.float32)).astype(jnp.bfloat16)
        later_state[h, :HEAD] = dot(c, upstream[:, at], CONTRACT_FIRST).astype(jnp.bfloat16)
        carry = jnp.where(
            meta[0:1, -1:] == meta[1:2, -1:], jnp.exp(sums[h : h + 1, -1:]), 0.0
        )
        carry = jnp.broadcast_to(carry, (EXTRA, HEAD)).astype(jnp.bfloat16)
        local_state[h, HEAD:] = carry
        later_state[h, HEAD:] = carry


def intra_kernel(query, keys, values, upstream, sums, meta, part_q, part_k, part_v):
    rows = meta.shape[1]
    causal = lax.broadcasted_iota(jnp.int32, (rows, rows), 0) >= lax.broadcasted_iota(
        jnp.int32, (rows, rows), 1
    )
    for h in range(sums.shape[0]):
        at = slice(h * HEAD, (h + 1) * HEAD)
        along, down, seg_along, seg_down = factors(sums, meta, h)
        same = causal & (seg_along == seg_down)
        decay = jnp.where(same, SCALE * jnp.exp(jnp.where(same, down - along, 0.0)), 0.0)
        q, k, v, u = query[:, at], keys[:, at], values[:, at], upstream[:, at]
        attn_qk = (decay * dot(q, k, CONTRACT_LAST)).astype(jnp.bfloat16)
        attn_up = (decay * dot(u, v, CONTRACT_LAST)).astype(jnp.bfloat16)
        part_q[:, at] = dot(attn_up, k)
        part_k[:, at] = dot(attn_up, q, CONTRACT_FIRST)
        part_v[:, at] = dot(attn_qk, u, CONTRACT_FIRST)


def chained(states, head):
    total = states[-1][head, :HEAD].astype(jnp.float32)
    for state in states[-2::-1]:
        own = state[head].astype(jnp.float32)
        total = own[:HEAD] + own[HEAD : HEAD + 1] * total
    return total.astype(jnp.bfloat16)


def make_inter_kernel(reach):
    def inter_kernel(*refs):
        keys, values, upstream, sums, meta, part_q, part_k, part_v = refs[:8]
        rest = refs[8:-1]
        earlier, later = rest[:reach], rest[reach:]
        grads = refs[-1]
        for h in range(sums.shape[0]):
            at = slice(h * HEAD, (h + 1) * HEAD)
            _, down, _, seg_down = factors(sums, meta, h)
            out = outflow_tile(down, seg_down, sums, meta, h)
            into = inflow_tile(down, seg_down, meta)
            incoming = chained(earlier, h)
            returning = chained(later, h)
            u, v, k = upstream[:, at], values[:, at], keys[:, at]
            grads[2, :, at] = (part_v[:, at] + out * dot(k, returning)).astype(jnp.bfloat16)
            grads[1, :, at] = (
                part_k[:, at] + out * dot(v, returning, CONTRACT_LAST)
            ).astype(jnp.bfloat16)
            grads[0, :, at] = (
                part_q[:, at] + into * dot(u, incoming, CONTRACT_LAST)
            ).astype(jnp.bfloat16)

    return inter_kernel


def call(kernel, outs, operands, flops):
    return pl.pallas_call(
        kernel,
        out_shape=outs,
        in_specs=[VMEM] * len(operands),
        out_specs=[VMEM] * len(outs),
        cost_estimate=pl.CostEstimate(flops=flops, bytes_accessed=4 << 20, transcendentals=0),
    )(*operands)


def shifted(x, offset, count):
    pairs = [(i, i + offset) for i in range(count) if 0 <= i + offset < count]
    return lax.ppermute(x, "seq", pairs)


def local(tokens, w_query, w_key, w_value, upstream, log_decay, segment):
    rows, part_width = tokens.shape
    width = w_query.shape[1]
    heads = width // HEAD
    head_count, count = lax.axis_size("head"), lax.axis_size("seq")
    my_head, my_index = lax.axis_index("head"), lax.axis_index("seq")

    token_parts = [tokens] + [
        lax.ppermute(tokens, "head", [(i, i ^ k) for i in range(head_count)])
        for k in range(1, head_count)
    ]

    first = my_index * rows
    segs = lax.dynamic_slice_in_dim(segment, first, rows)
    before = lax.dynamic_slice_in_dim(segment, jnp.maximum(first - 1, 0), 1)[0]
    previous = jnp.where(my_index > 0, before, jnp.int32(-1))
    upper = jnp.triu(jnp.ones((rows, rows), jnp.float32))
    sums = lax.dot_general(
        log_decay, upper, CONTRACT_FIRST, precision=lax.Precision.HIGHEST,
        preferred_element_type=jnp.float32,
    )
    meta = jnp.stack([segs, jnp.full_like(segs, previous)]).astype(jnp.float32)

    longest = segment.shape[0] // 4
    reach = min((longest - 1) // rows + 1, count - 1)

    def project(weight):
        total = None
        for k, part in enumerate(token_parts):
            start = (my_head ^ k) * part_width
            term = dot(part, lax.dynamic_slice_in_dim(weight, start, part_width))
            total = term if total is None else total + term
        return total.astype(jnp.bfloat16)

    query, keys, values = project(w_query), project(w_key), project(w_value)

    square = jax.ShapeDtypeStruct((heads, HEAD + EXTRA, HEAD), jnp.bfloat16)
    flat_float = jax.ShapeDtypeStruct((rows, width), jnp.float32)
    triple = jax.ShapeDtypeStruct((3, rows, width), jnp.bfloat16)
    one = 2 * rows * HEAD * width
    shared = [query, keys, values, upstream, sums, meta]
    local_state, later_state = call(states_kernel, [square] * 2, shared, 2 * one)
    earlier = [shifted(local_state, j, count) for j in range(1, reach + 1)]
    later = [shifted(later_state, -j, count) for j in range(1, reach + 1)]
    parts = call(intra_kernel, [flat_float] * 3, shared, 5 * one)

    chips = count // 2
    chip, core = my_index // 2, my_index % 2
    own_width = part_width * head_count // count
    per_part = part_width // own_width
    stacked = jnp.stack(token_parts)

    def columns_for(place):
        return lax.dynamic_slice(
            stacked,
            ((place // per_part) ^ my_head, 0, (place % per_part) * own_width),
            (1, rows, own_width),
        )[0]

    partner = [(i, i ^ 1) for i in range(count)]
    places = [2 * ((chip + d) % chips) for d in range(chips)]
    kept = [columns_for(place + core) for place in places]
    given = jnp.stack([columns_for(place + 1 - core) for place in places])
    taken = lax.ppermute(given, "seq", partner)
    columns = []
    for d in range(chips):
        block = jnp.concatenate([kept[d], taken[d]], axis=0)
        if d:
            block = lax.ppermute(block, "seq", [(i, (i + 2 * d) % count) for i in range(count)])
        columns.append(block)

    (grads,) = call(
        make_inter_kernel(reach), [triple],
        [keys, values, upstream, sums, meta, *parts, *earlier, *later],
        3 * one,
    )
    columns, _ = lax.optimization_barrier((columns, grads))

    ahead = [(i, (i + 2) % count) for i in range(count)]
    behind = [(i, (i - 2) % count) for i in range(count)]
    middle = chips // 2
    found = {0: grads}
    right = left = grads
    for d in range(1, middle):
        right = lax.ppermute(right, "seq", ahead)
        left = lax.ppermute(left, "seq", behind)
        found[d], found[chips - d] = right, left
    half = rows // 2
    halves = [
        lax.ppermute(right[:, :half], "seq", ahead),
        lax.ppermute(left[:, half:], "seq", behind),
    ]
    found = {d: [x, lax.ppermute(x, "seq", partner)] for d, x in found.items()}
    halves = [(x, lax.ppermute(x, "seq", partner)) for x in halves]
    near = sorted(found)
    near_columns = jnp.concatenate([columns[d] for d in near], axis=0)

    outs = []
    for i in range(3):
        block = jnp.concatenate([x[i] for d in near for x in found[d]], axis=0)
        total = dot(near_columns, block, CONTRACT_FIRST)
        far = jnp.concatenate([x[p][i] for p in range(2) for x in halves], axis=0)
        total = total + dot(columns[middle], far, CONTRACT_FIRST)
        outs.append(total.astype(jnp.bfloat16))
    return tuple(outs)


def solution(mesh):
    placed = (
        P("seq", "head"),
        P(None, "head"),
        P(None, "head"),
        P(None, "head"),
        P("seq", "head"),
        P("seq", "head"),
        P(),
    )
    return jax.shard_map(
        local,
        mesh=mesh,
        in_specs=placed,
        out_specs=(P("seq", "head"), P("seq", "head"), P("seq", "head")),
        check_vma=False,
    )
```
